32 devices in a mesh: tm: 8 (over z, x), rows: 4 (over y, core).
Axes of the slice: x: 2, y: 2, z: 4, core: 2. Of those that a mesh axis runs over, the one named last changes fastest.
Arguments:
- initial_warmth: float32 [1024, 1024], P('rows'), may hold values from -6 to 6
- pattern_choice: int32 [16, 8, 8], P('tm'), may hold values from 0 to 7
- dissipation_tables: float32 [8, 128, 128], replicated, may hold values from -6 to 6
- material_label: int32 [8, 8], replicated, may hold values from 0 to 3
- intercept_kappa: float32 [4], replicated, may hold values from 4 to 8
- sensitivity_coef: float32 [4], replicated, may hold values from -0.5 to 0.5
Outputs:
- warmth_trajectory: float32 [16, 1024, 1024], P('tm', 'rows')
The draws below stay inside these ranges and needn't reach their ends.
All inputs are finite; a program needn't handle non-finite values.
Results may differ from the reference program's by a relative error of at most 0.0003.
Values sent between devices are 32-bit elements; how exact they have to be, the bound alone decides.
A program may use at most 128 MiB of HBM per device.

```python
import math
import jax
import jax.numpy as jnp
from jax import lax

TILES_PER_ROW = 1024
TILES_PER_COLUMN = 1024
TILE = 128
REGIONS = 4
PATTERNS = 8
ITERS = 2
HORIZON_COUNT = 16
TY = 8
TX = 8


def draw_pattern_choice(key, part):
    base_key = jax.random.fold_in(key, 101)
    fresh_key = jax.random.fold_in(key, 202)
    switch_key = jax.random.fold_in(key, 303)
    settled = jax.random.randint(base_key, (TY, TX), 0, PATTERNS)
    fresh = jax.random.randint(fresh_key, (HORIZON_COUNT, TY, TX), 0, PATTERNS)
    switch = jax.random.randint(switch_key, (HORIZON_COUNT, TY, TX), 0, 4)
    return jnp.where(switch == 0, fresh, settled[None]).astype(jnp.int32)


def draw_dissipation_tables(key, part):
    rough_key = jax.random.fold_in(key, 404)
    rough = jax.random.normal(rough_key, (PATTERNS, TILE, TILE), jnp.float32)
    return jnp.clip(rough, -6.0, 6.0).astype(jnp.float32)


def touch_ends(array, key, smallest, top_value):
    spot = [jax.random.randint(jax.random.fold_in(key, axis), (), 0, length) for axis, length in enumerate(array.shape)]
    widest = array.shape.index(max(array.shape))
    neighbour = spot[:widest] + [(spot[widest] + 1) % array.shape[widest]] + spot[widest + 1:]
    return array.at[tuple(spot)].set(smallest).at[tuple(neighbour)].set(top_value)


def level_of(stream_key, extent, cuts, least, largest):
    def one(position, shards_of):
        steps = jax.random.uniform(jax.random.fold_in(jax.random.fold_in(stream_key, 6), position), (shards_of,), jnp.float32, least / len(cuts), largest / len(cuts))
        return jnp.repeat(jnp.exp(steps), extent[position] // shards_of).reshape((-1,) + (1,) * (len(extent) - position - 1))

    factor_of = one(*cuts[0])
    for cut in cuts[1:]:
        factor_of = factor_of * one(*cut)
    return factor_of


def scatter_about(rng, shape, spread, most, cuts=(), kind=jnp.bfloat16):
    drawn = spread * jax.random.normal(rng, shape, jnp.float32)
    if cuts:
        drawn = drawn * level_of(rng, shape, cuts, -0.22, 0.18)
    return jnp.clip(drawn, -most, most).astype(kind)


def setup_inputs(seed: int = 0) -> dict:
    key_of = jax.random.split(jax.random.key(seed), 7)
    return {
        "initial_warmth": scatter_about(key_of[0], (TILES_PER_COLUMN, TILES_PER_ROW), 1.0, 6.0, ((0, 4),), jnp.float32),
        "pattern_choice": draw_pattern_choice(jax.random.fold_in(key_of[6], 71), 0),
        "dissipation_tables": draw_dissipation_tables(jax.random.fold_in(key_of[6], 71), 0),
        "material_label": touch_ends(jax.random.randint(key_of[3], (TY, TX), 0, REGIONS), jax.random.fold_in(key_of[3], 1), 0, REGIONS - 1).astype(jnp.int32),
        "intercept_kappa": jnp.clip(jnp.exp(jax.random.uniform(key_of[4], (REGIONS,), jnp.float32, math.log(4.0), math.log(8.0))), 4.0, 8.0),
        "sensitivity_coef": jnp.clip(jax.random.uniform(key_of[5], (REGIONS,), jnp.float32, -0.5, 0.5), -0.5, 0.5),
    }


TIMESTEP_SIZE = 2.0
ALPHA = 0.05
CROSS_WEIGHT = 1.0 / 64.0


def dct_last(values):
    count = values.shape[-1]
    mirrored = jnp.concatenate([values, jnp.flip(values, -1)], -1)
    spectrum = jnp.fft.fft(mirrored, axis=-1)[..., :count]
    angle = jnp.arange(count).astype(values.dtype) * (math.pi / (2 * count))
    return 0.5 * (jnp.real(spectrum) * jnp.cos(angle) + jnp.imag(spectrum) * jnp.sin(angle))


def idct_last(values):
    count = values.shape[-1]
    angle = jnp.arange(count).astype(values.dtype) * (math.pi / (2 * count))
    weights = jnp.where(jnp.arange(count) == 0, 1.0, 2.0).astype(values.dtype)
    scaled = values * weights
    filled = lax.complex(scaled * jnp.cos(angle), scaled * jnp.sin(angle))
    filled = jnp.concatenate([filled, jnp.zeros_like(filled)], -1)
    return 2.0 * jnp.real(jnp.fft.ifft(filled, axis=-1))[..., :count]


def both_forward(values):
    inner = dct_last(values)
    return jnp.swapaxes(dct_last(jnp.swapaxes(inner, 1, 2)), 1, 2)


def both_inverse(values):
    inner = jnp.swapaxes(idct_last(jnp.swapaxes(values, 1, 2)), 1, 2)
    return idct_last(inner)


def reference(initial_warmth, pattern_choice, dissipation_tables, material_label, intercept_kappa, sensitivity_coef):
    tiles = dissipation_tables[pattern_choice]
    forcing_term = jnp.transpose(tiles, (0, 1, 3, 2, 4)).reshape(HORIZON_COUNT, TILES_PER_COLUMN, TILES_PER_ROW)
    reference_level = jnp.repeat(jnp.repeat(intercept_kappa[material_label], TILE, 0), TILE, 1)
    kappa_derivative = jnp.repeat(jnp.repeat(sensitivity_coef[material_label], TILE, 0), TILE, 1)
    conduct = jnp.mean(intercept_kappa)
    amplification = jnp.exp(jnp.arange(HORIZON_COUNT).astype(jnp.float32) * (math.log(ALPHA) / HORIZON_COUNT))
    shrink = ALPHA ** (1.0 / HORIZON_COUNT)
    theta = jnp.arange(HORIZON_COUNT).astype(jnp.float32) * (2.0 * math.pi / HORIZON_COUNT)
    mu_rows = 2.0 - 2.0 * jnp.cos(jnp.arange(TILES_PER_COLUMN).astype(jnp.float32) * (math.pi / TILES_PER_COLUMN))
    mu_cols = 2.0 - 2.0 * jnp.cos(jnp.arange(TILES_PER_ROW).astype(jnp.float32) * (math.pi / TILES_PER_ROW))
    real_den = (1.0 - shrink * jnp.cos(theta))[:, None, None] / TIMESTEP_SIZE + conduct * (mu_rows[None, :, None] + CROSS_WEIGHT * mu_cols[None, None, :])
    imag_den = (shrink * jnp.sin(theta) / TIMESTEP_SIZE)[:, None, None]
    norm_den = real_den * real_den + imag_den * imag_den
    warmth_trajectory = jnp.broadcast_to(initial_warmth[None], (HORIZON_COUNT, TILES_PER_COLUMN, TILES_PER_ROW)).astype(jnp.float32)
    for sweep in range(ITERS):
        kappa_local = reference_level * (1.0 + kappa_derivative * jnp.tanh(warmth_trajectory))
        upward_current = 0.5 * (kappa_local[:, 1:] + kappa_local[:, :-1]) * (warmth_trajectory[:, 1:] - warmth_trajectory[:, :-1])
        lateral_current = CROSS_WEIGHT * (0.5 * (kappa_local[:, :, 1:] + kappa_local[:, :, :-1]) * (warmth_trajectory[:, :, 1:] - warmth_trajectory[:, :, :-1]))
        energy_ledger = jnp.pad(upward_current, ((0, 0), (0, 1), (0, 0))) - jnp.pad(upward_current, ((0, 0), (1, 0), (0, 0)))
        energy_ledger = energy_ledger + jnp.pad(lateral_current, ((0, 0), (0, 0), (0, 1))) - jnp.pad(lateral_current, ((0, 0), (0, 0), (1, 0)))
        former_warmth = jnp.concatenate([initial_warmth[None], warmth_trajectory[:-1]], 0)
        defect_vector = forcing_term - (warmth_trajectory - former_warmth) / TIMESTEP_SIZE + energy_ledger
        scaled = defect_vector * amplification[:, None, None]
        spectrum = jnp.fft.fft(scaled, axis=0)
        modes_re = both_forward(jnp.real(spectrum))
        modes_im = both_forward(jnp.imag(spectrum))
        solved_re = (modes_re * real_den + modes_im * imag_den) / norm_den
        solved_im = (modes_im * real_den - modes_re * imag_den) / norm_den
        field_re = both_inverse(solved_re)
        field_im = both_inverse(solved_im)
        correction_delta = jnp.real(jnp.fft.ifft(lax.complex(field_re, field_im), axis=0))
        warmth_trajectory = warmth_trajectory + correction_delta / amplification[:, None, None]
    return warmth_trajectory
```

```python
import math

import jax
import jax.numpy as jnp
import numpy as np
from jax import lax
from jax.experimental import pallas as pl
from jax.experimental.pallas import tpu as pltpu
from jax.sharding import PartitionSpec as P

TILE = 128
ITERS = 2
TIMESTEP_SIZE = 2.0
ALPHA = 0.05
CROSS_WEIGHT = 1.0 / 64.0
F32 = jnp.float32
BF16 = jnp.bfloat16


def extended(block, axis, dim):
    count = lax.axis_size(axis)
    forward = [(i, i + 1) for i in range(count - 1)]
    backward = [(target, source) for source, target in forward]
    low = lax.ppermute(
        lax.slice_in_dim(block, block.shape[dim] - 1, None, axis=dim), axis, forward
    )
    high = lax.ppermute(lax.slice_in_dim(block, 0, 1, axis=dim), axis, backward)
    return jnp.concatenate([low, block, high], axis=dim)


def cosine_table(length):
    modes = np.arange(length, dtype=np.int64)[:, None]
    cells = np.arange(length, dtype=np.int64)[None, :]
    phase = modes * (2 * cells + 1) % (4 * length)
    return np.cos(phase * (math.pi / (2 * length)))


def two_parts(table):
    high = np.asarray(table, dtype=np.float32).astype(BF16)
    low = (table - high.astype(np.float64)).astype(np.float32).astype(BF16)
    return jnp.asarray(high), jnp.asarray(low)


def split(values):
    high = values.astype(BF16)
    return high, (values - high.astype(F32)).astype(BF16)


def mul(left, right):
    return jnp.dot(left, right, preferred_element_type=F32)


def columns_kernel(x_ref, high_ref, low_ref, out_ref, x_high, x_low):
    @pl.when(pl.program_id(0) == 0)
    def _():
        x_high[...], x_low[...] = split(x_ref[...])

    high = high_ref[...]
    out_ref[...] = (
        mul(x_high[...], high) + mul(x_low[...], high) + mul(x_high[...], low_ref[...])
    )


def times_table(values, table):
    rows, depth = values.shape
    width = table[0].shape[1]
    block = min(256, width)
    return pl.pallas_call(
        columns_kernel,
        grid=(width // block,),
        out_shape=jax.ShapeDtypeStruct((rows, width), F32),
        in_specs=[
            pl.BlockSpec((rows, depth), lambda i: (0, 0)),
            pl.BlockSpec((depth, block), lambda i: (0, i)),
            pl.BlockSpec((depth, block), lambda i: (0, i)),
        ],
        out_specs=pl.BlockSpec((rows, block), lambda i: (0, i)),
        scratch_shapes=[pltpu.VMEM((rows, depth), BF16)] * 2,
    )(values, *table)


def rows_kernel(high_ref, low_ref, x_ref, out_ref, x_high, x_low):
    @pl.when(pl.program_id(0) == 0)
    def _():
        x_high[...], x_low[...] = split(x_ref[...])

    for n in range(x_ref.shape[0]):
        out_ref[n] = (
            mul(high_ref[...], x_high[n])
            + mul(high_ref[...], x_low[n])
            + mul(low_ref[...], x_high[n])
        )


def table_times(table, values):
    steps, depth, width = values.shape
    height = table[0].shape[0]
    block = min(256, height)
    return pl.pallas_call(
        rows_kernel,
        grid=(height // block,),
        out_shape=jax.ShapeDtypeStruct((steps, height, width), F32),
        in_specs=[
            pl.BlockSpec((block, depth), lambda i: (i, 0)),
            pl.BlockSpec((block, depth), lambda i: (i, 0)),
            pl.BlockSpec((steps, depth, width), lambda i: (0, 0, 0)),
        ],
        out_specs=pl.BlockSpec((steps, block, width), lambda i: (0, i, 0)),
        scratch_shapes=[pltpu.VMEM((steps, depth, width), BF16)] * 2,
    )(*table, values)


def power_kernel(choice_ref, table_ref, out_ref):
    steps, blocks, _, width = out_ref.shape
    across = width // TILE
    for n in range(steps):
        for b in range(blocks):
            for x in range(across):
                picked = choice_ref[n, b * across + x]
                out_ref[n, b, :, x * TILE : (x + 1) * TILE] = table_ref[picked]


def power_of(pattern_choice, tables, first_row, strip, width):
    steps = pattern_choice.shape[0]
    part = min(TILE, strip)
    blocks = strip // part
    offset = first_row % TILE if strip < TILE else 0
    tiles = lax.dynamic_slice_in_dim(tables, offset, part, axis=1)
    chosen = lax.dynamic_slice_in_dim(pattern_choice, first_row // TILE, blocks, axis=1)
    power = pl.pallas_call(
        power_kernel,
        out_shape=jax.ShapeDtypeStruct((steps, blocks, part, width), F32),
        in_specs=[
            pl.BlockSpec(memory_space=pltpu.SMEM),
            pl.BlockSpec(memory_space=pltpu.VMEM),
        ],
        out_specs=pl.BlockSpec(memory_space=pltpu.VMEM),
    )(chosen.reshape(steps, -1), tiles)
    return power.reshape(steps, strip, width)


def divergence(warmth, kappa, inner):
    def face(low, high):
        return 1.0 if kappa is None else 0.5 * (low + high)

    k = warmth if kappa is None else kappa
    upward = face(k[:, 1:], k[:, :-1]) * (warmth[:, 1:] - warmth[:, :-1])
    upward = jnp.where(inner[None, :, None], upward, 0.0)
    centre, k_mid = warmth[:, 1:-1], k[:, 1:-1]
    lateral = CROSS_WEIGHT * (
        face(k_mid[:, :, 1:], k_mid[:, :, :-1]) * (centre[:, :, 1:] - centre[:, :, :-1])
    )
    zero = jnp.zeros_like(centre[:, :, :1])
    across = jnp.concatenate([lateral, zero], 2) - jnp.concatenate([zero, lateral], 2)
    return upward[:, 1:] - upward[:, :-1] + across


def mode_factors(row_ids, column_ids, height, width, conduct):
    mu_rows = 2.0 - 2.0 * jnp.cos(row_ids.astype(F32) * (math.pi / height))
    mu_cols = 2.0 - 2.0 * jnp.cos(column_ids.astype(F32) * (math.pi / width))
    rate = conduct * (mu_rows[:, None] + CROSS_WEIGHT * mu_cols[None, :])
    gain = 1.0 / (1.0 / TIMESTEP_SIZE + rate)
    return gain, gain * (1.0 / TIMESTEP_SIZE)


def shards(
    initial_warmth,
    pattern_choice,
    dissipation_tables,
    material_label,
    intercept_kappa,
    sensitivity_coef,
):
    steps = pattern_choice.shape[0]
    strip, width = initial_warmth.shape
    tm_count = lax.axis_size("tm")
    rows_count = lax.axis_size("rows")
    height = strip * rows_count
    first_row = lax.axis_index("rows") * strip
    power = power_of(pattern_choice, dissipation_tables, first_row, strip, width)

    padded_rows = first_row - 1 + jnp.arange(strip + 2, dtype=jnp.int32)
    labels = jnp.take(material_label, jnp.clip(padded_rows, 0, height - 1) // TILE, axis=0)
    base_tiles = jnp.zeros(labels.shape, F32)
    slope_tiles = jnp.zeros(labels.shape, F32)
    for label in range(intercept_kappa.shape[0]):
        base_tiles = jnp.where(labels == label, intercept_kappa[label], base_tiles)
        slope_tiles = jnp.where(labels == label, sensitivity_coef[label], slope_tiles)
    base = jnp.repeat(base_tiles, TILE, axis=1)[None]
    slope = jnp.repeat(slope_tiles, TILE, axis=1)[None]
    upper_rows = padded_rows[:-1]
    inner = (upper_rows >= 0) & (upper_rows + 1 <= height - 1)
    conduct = jnp.mean(intercept_kappa)

    column_cos = cosine_table(width)
    row_cos = cosine_table(height)
    columns_out, columns_in = two_parts(column_cos.T), two_parts(column_cos)
    if height == width:
        rows_out, rows_in = columns_in, columns_out
    else:
        rows_out, rows_in = two_parts(row_cos), two_parts(row_cos.T)

    narrow = width // rows_count
    share = height // tm_count
    column_ids = lax.axis_index("rows") * narrow + jnp.arange(narrow, dtype=jnp.int32)
    all_rows = jnp.arange(height, dtype=jnp.int32)
    own_rows = lax.axis_index("tm") * share + jnp.arange(share, dtype=jnp.int32)
    gain, keep = mode_factors(all_rows, column_ids, height, width, conduct)
    weight = (jnp.where(all_rows == 0, 1.0, 2.0) / height)[:, None] * (
        jnp.where(column_ids == 0, 1.0, 2.0) / width
    )[None, :]
    _, own_keep = mode_factors(own_rows, column_ids, height, width, conduct)
    block_keep = own_keep
    for _ in range(steps - 1):
        block_keep = block_keep * own_keep
    around = block_keep
    for _ in range(tm_count - 1):
        around = around * block_keep
    closing = ALPHA / (1.0 - ALPHA * around)
    first_block = lax.axis_index("tm") == 0

    start = extended(initial_warmth[None], "rows", 1)
    start_div = divergence(start, base * (1.0 + slope * jnp.tanh(start)), inner)
    warmth = jnp.broadcast_to(initial_warmth[None], (steps, strip, width))
    wrapped = None
    for sweep in range(ITERS):
        if sweep == 0:
            resid = power + start_div
        else:
            grid = extended(warmth, "rows", 1)
            div = divergence(grid, base * (1.0 + slope * jnp.tanh(grid)), inner)
            resid = div - last_div - conduct * divergence(grid - last_grid, None, inner)
        modes = times_table(resid.reshape(steps * strip, width), columns_out)
        modes = lax.all_to_all(
            modes.reshape(steps, strip, width), "rows", split_axis=2, concat_axis=1, tiled=True
        )
        modes = table_times(rows_out, modes)
        sources = [modes[n] * weight for n in range(steps)]
        if wrapped is not None:
            sources[0] = sources[0] - jnp.where(first_block, wrapped / TIMESTEP_SIZE, 0.0)
        sources = [gain * source for source in sources]
        block_end = sources[0]
        for source in sources[1:]:
            block_end = source + keep * block_end
        ends = lax.all_to_all(block_end, "tm", split_axis=0, concat_axis=0, tiled=True)
        ends = ends.reshape(tm_count, share, narrow)
        last = ends[0]
        for k in range(1, tm_count):
            last = ends[k] + block_keep * last
        entry = [closing * last]
        for k in range(tm_count - 1):
            entry.append(ends[k] + block_keep * entry[k])
        entry = jnp.concatenate(entry, 0)
        carry = lax.all_to_all(entry, "tm", split_axis=0, concat_axis=0, tiled=True)
        wrapped = carry
        solved = []
        for source in sources:
            carry = source + keep * carry
            solved.append(carry)
        field = table_times(rows_in, jnp.stack(solved, 0))
        field = lax.all_to_all(field, "rows", split_axis=1, concat_axis=2, tiled=True)
        update = times_table(field.reshape(steps * strip, width), columns_in)
        if sweep == 0:
            last_grid, last_div = start, start_div
        else:
            last_grid, last_div = grid, div
        warmth = warmth + update.reshape(steps, strip, width)
    return warmth


def solution(mesh):
    in_specs = (P("rows", None), P("tm", None, None), P(), P(), P(), P())
    out_specs = P("tm", "rows", None)
    return jax.shard_map(shards, mesh=mesh, in_specs=in_specs, out_specs=out_specs, check_vma=False)
```
